32 devices in a mesh: band: 2 (over x), vis: 16 (over z, y, core).
Axes of the slice: x: 2, y: 2, z: 4, core: 2. Of those that a mesh axis runs over, the one named last changes fastest.
Arguments:
- sky_image: float32 [4096, 4096], P(('band', 'vis')), as said below
- coef_dual: float32 [4, 2048, 2048], P(None, ('band', 'vis')), may hold values from -12 to 12
- vis_dual: float32 [2, 16, 16, 4, 2, 32], P('band', 'vis'), may hold values from -12 to 12
- visibilities: float32 [2, 16, 16, 4, 2, 32], P('band', 'vis')
- kernel_blocks: bfloat16 [2, 16, 16, 4, 2, 32, 256], P('band', 'vis'), may hold values from -0.375 to 0.375
- tile_rows: int32 [2, 16, 16, 4], P('band', 'vis'), may hold values from 0 to 2047
- tile_counts: int32 [2, 16, 16], P('band', 'vis'), may hold values from 1 to 4, as said below
Outputs:
- new_image: float32 [4096, 4096], P(('band', 'vis'))
- new_coef_dual: float32 [4, 2048, 2048], P(None, ('band', 'vis'))
- new_vis_dual: float32 [2, 16, 16, 4, 2, 32], P('band', 'vis')
The draws below stay inside these ranges and needn't reach their ends.
Inputs may be any that keep to these rules, and one draw needn't show every extreme that they name: `sky_image`: nonnegative. `tile_counts`: in every band some owner q has all 4 slots live from every device of that band.
All inputs are finite; a program needn't handle non-finite values.
Results may differ from the reference program's by a relative error of at most 0.0018.
Values may be sent and summed in bfloat16 or wider, within the bound.
A program may use at most 128 MiB of HBM per device.

```python
import jax
import jax.numpy as jnp
from jax import lax

IMG = 4096
VT = 32
SLOTS = 4
ITERS = 1
STRIPE = 2048
PIECE_ROWS = 256
HALF = 2048
N_BAND = 2
N_VIS = 16


def draw_sky_image(key, part):
    row_key, col_key, base_key = jax.random.split(key, 3)
    row_scale = jnp.exp(jax.random.uniform(row_key, (IMG, 1), jnp.float32) * jnp.log(10.0))
    col_scale = jnp.exp(jax.random.uniform(col_key, (1, IMG), jnp.float32) * jnp.log(10.0))
    rising = 1.0 + 2.0 * jnp.arange(IMG, dtype=jnp.float32)[:, None] / IMG
    base_values = jax.random.uniform(base_key, (IMG, IMG), jnp.float32)
    return 0.2 * base_values * row_scale * col_scale * rising


def draw_visibilities(key, part):
    full_shape = (N_BAND, N_VIS, N_VIS, SLOTS, 2, VT)
    scale_key, value_key = jax.random.split(key)
    tile_scale = jnp.exp(jax.random.uniform(scale_key, (N_BAND, N_VIS, N_VIS, SLOTS, 1, 1), jnp.float32) * jnp.log(10.0))
    position = (jnp.arange(N_BAND * N_VIS, dtype=jnp.float32) / (N_BAND * N_VIS - 1)).reshape(N_BAND, N_VIS, 1, 1, 1, 1)
    values = jax.random.normal(value_key, full_shape, jnp.float32)
    rising = 1.0 + 2.0 * position
    return values * tile_scale * rising


def draw_tile_counts(key, part):
    count_key, owner_key = jax.random.split(jax.random.fold_in(key, 11))
    counts = jax.random.randint(count_key, (N_BAND, N_VIS, N_VIS), 1, SLOTS + 1)
    full_owner = jax.random.randint(owner_key, (N_BAND, 1, 1), 0, N_VIS)
    owners = jnp.arange(N_VIS, dtype=jnp.int32)[None, None, :]
    return jnp.where(owners == full_owner, SLOTS, counts).astype(jnp.int32)


def plant(values, key, low, largest):
    extent = values.shape
    spot = [jax.random.randint(jax.random.fold_in(key, axis), (), 0, extent[axis]) for axis in range(len(extent))]
    values = values.at[tuple(spot)].set(low)
    longest = extent.index(max(extent))
    spot[longest] = (spot[longest] + 1) % extent[longest]
    return values.at[tuple(spot)].set(largest)


def block_levels(rng, shape, cuts, least, largest):
    loudness, own = 1.0, jax.random.fold_in(rng, 6)
    for dim, shards_of in cuts:
        heights = jnp.exp(jax.random.uniform(jax.random.fold_in(own, dim), (shards_of,), jnp.float32, least / len(cuts), largest / len(cuts)))
        loudness = loudness * jnp.repeat(heights, shape[dim] // shards_of).reshape([-1 if axis == dim else 1 for axis in range(len(shape))])
    return loudness


def centred(own_key, extent, width, limit, cuts=(), held_as=jnp.bfloat16):
    entries = width * jax.random.normal(own_key, extent, jnp.float32)
    if cuts:
        entries = entries * block_levels(own_key, extent, cuts, -0.22, 0.18)
    return jnp.clip(entries, -limit, limit).astype(held_as)


def setup_inputs(seed: int = 0) -> dict:
    splits = jax.random.split(jax.random.key(seed), 8)
    sky_image = draw_sky_image(jax.random.fold_in(splits[7], 71), 0)
    coef_dual = centred(splits[1], (4, HALF, HALF), 2.0, 12.0, ((1, 32),), jnp.float32)
    vis_dual = centred(splits[2], (N_BAND, N_VIS, N_VIS, SLOTS, 2, VT), 2.0, 12.0, ((0, 2), (1, 16)), jnp.float32)
    visibilities = draw_visibilities(jax.random.fold_in(splits[7], 71), 0)
    kernel_blocks = centred(splits[4], (N_BAND, N_VIS, N_VIS, SLOTS, 2, VT, PIECE_ROWS), PIECE_ROWS ** -0.5, 0.375, ((0, 2), (1, 16)))
    tile_rows = plant(jax.random.randint(splits[5], (N_BAND, N_VIS, N_VIS, SLOTS), 0, STRIPE), jax.random.fold_in(splits[5], 1), 0, STRIPE - 1).astype(jnp.int32)
    tile_counts = draw_tile_counts(jax.random.fold_in(splits[7], 71), 0)
    return dict(sky_image=sky_image, coef_dual=coef_dual, vis_dual=vis_dual, visibilities=visibilities, kernel_blocks=kernel_blocks, tile_rows=tile_rows, tile_counts=tile_counts)


low_taps = (-0.010597401784997278, 0.032883011666982945, 0.030841381835986965, -0.18703481171888114, -0.02798376941698385, 0.6308807679295904, 0.7148465705525415, 0.23037781330885523)
high_taps = tuple(((-1.0) ** offset * low_taps[7 - offset] for offset in range(8)))
highest = lax.Precision.HIGHEST

def analyse_axis(field, axis):
    length = field.shape[axis]
    low_part = 0.0
    high_part = 0.0
    for offset in range(8):
        taken = lax.slice_in_dim(jnp.roll(field, -offset, axis=axis), 0, length, 2, axis)
        low_part = low_part + low_taps[offset] * taken
        high_part = high_part + high_taps[offset] * taken
    return (low_part, high_part)

def synthesise_axis(low_part, high_part, axis):
    halves = []
    for parity in range(2):
        summed = 0.0
        for delay in range(4):
            summed = summed + low_taps[parity + 2 * delay] * jnp.roll(low_part, delay, axis=axis)
            summed = summed + high_taps[parity + 2 * delay] * jnp.roll(high_part, delay, axis=axis)
        halves.append(summed)
    joined = jnp.stack(halves, axis=axis + 1)
    new_shape = list(low_part.shape)
    new_shape[axis] = 2 * new_shape[axis]
    return joined.reshape(new_shape)

def analysis(field):
    rows_low, rows_high = analyse_axis(field, 0)
    low_low, low_high = analyse_axis(rows_low, 1)
    high_low, high_high = analyse_axis(rows_high, 1)
    return jnp.stack([low_low, low_high, high_low, high_high])

def synthesis(coeffs):
    rows_low = synthesise_axis(coeffs[0], coeffs[1], 1)
    rows_high = synthesise_axis(coeffs[2], coeffs[3], 1)
    return synthesise_axis(rows_low, rows_high, 0)

def forward_map(extrap, kernel_blocks, tile_rows):
    spectrum = jnp.fft.fft2(extrap) / IMG
    flipped = spectrum.T.reshape(N_BAND, STRIPE, N_VIS, PIECE_ROWS)
    real_grid = lax.optimization_barrier(jnp.real(flipped).astype(jnp.bfloat16))
    imag_grid = lax.optimization_barrier(jnp.imag(flipped).astype(jnp.bfloat16))
    owners = jnp.arange(N_VIS, dtype=jnp.int32)[None, :, None]

    def per_band(inputs):
        kernels, rows_band, real_band, imag_band = inputs
        tile_real = real_band[rows_band, owners].astype(jnp.float32)
        tile_imag = imag_band[rows_band, owners].astype(jnp.float32)
        kernel_real = kernels[:, :, :, 0].astype(jnp.float32)
        kernel_imag = kernels[:, :, :, 1].astype(jnp.float32)
        out_real = jnp.einsum('vqsat,vqst->vqsa', kernel_real, tile_real, precision=highest) - jnp.einsum('vqsat,vqst->vqsa', kernel_imag, tile_imag, precision=highest)
        out_imag = jnp.einsum('vqsat,vqst->vqsa', kernel_real, tile_imag, precision=highest) + jnp.einsum('vqsat,vqst->vqsa', kernel_imag, tile_real, precision=highest)
        return jnp.stack([out_real, out_imag], axis=3)
    return lax.map(per_band, (kernel_blocks, tile_rows, real_grid, imag_grid))

def adjoint_map(weights, kernel_blocks, tile_rows):
    rounded = lax.optimization_barrier(weights.astype(jnp.bfloat16))
    owners = jnp.arange(N_VIS, dtype=jnp.int32)[None, :, None]

    def per_band(inputs):
        kernels, rows_band, vis_band = inputs
        kernel_real = kernels[:, :, :, 0].astype(jnp.float32)
        kernel_imag = kernels[:, :, :, 1].astype(jnp.float32)
        weight_real = vis_band[:, :, :, 0].astype(jnp.float32)
        weight_imag = vis_band[:, :, :, 1].astype(jnp.float32)
        grid_real = jnp.einsum('vqsat,vqsa->vqst', kernel_real, weight_real, precision=highest) + jnp.einsum('vqsat,vqsa->vqst', kernel_imag, weight_imag, precision=highest)
        grid_imag = jnp.einsum('vqsat,vqsa->vqst', kernel_real, weight_imag, precision=highest) - jnp.einsum('vqsat,vqsa->vqst', kernel_imag, weight_real, precision=highest)
        stacked = jnp.stack([grid_real, grid_imag], axis=3)
        segment = (owners * STRIPE + rows_band).astype(jnp.int32)
        summed = jax.ops.segment_sum(stacked.reshape(-1, 2, PIECE_ROWS), segment.reshape(-1), num_segments=N_VIS * STRIPE)
        return summed.reshape(N_VIS, STRIPE, 2, PIECE_ROWS)
    grids = lax.map(per_band, (kernel_blocks, tile_rows, rounded))
    ordered = jnp.transpose(grids, (3, 1, 4, 0, 2)).reshape(2, IMG, IMG)
    spectrum = lax.complex(ordered[0], ordered[1])
    return jnp.real(jnp.fft.ifft2(spectrum)) * IMG

def reference(sky_image, coef_dual, vis_dual, visibilities, kernel_blocks, tile_rows, tile_counts):
    slot_index = jnp.arange(SLOTS, dtype=jnp.int32)
    live_slots = (slot_index < tile_counts[..., None]).astype(jnp.float32)[..., None, None]
    data_square = jnp.sum(live_slots * visibilities * visibilities)
    radius = 0.5 * jnp.sqrt(data_square + 1e-06)
    for iteration in range(ITERS):
        adjoint_part = adjoint_map(live_slots * vis_dual, kernel_blocks, tile_rows)
        smooth = synthesis(coef_dual)
        new_image = jnp.maximum(sky_image - smooth - adjoint_part, 0.0)
        extrap = 2.0 * new_image - sky_image
        coeffs = analysis(extrap)
        threshold = 0.5 * jnp.sum(jnp.abs(coeffs)) / (IMG * IMG)
        coef_dual = jnp.clip(coef_dual + coeffs, -threshold, threshold)
        predicted = forward_map(extrap, kernel_blocks, tile_rows)
        residual = live_slots * (vis_dual + predicted - visibilities)
        size_value = jnp.sqrt(jnp.sum(residual * residual) + 1e-06)
        vis_dual = residual * (1.0 - jnp.minimum(1.0, radius / size_value))
        sky_image = new_image
    return (sky_image, coef_dual, vis_dual)
```

```python
import math

import jax
import numpy as np
import jax.numpy as jnp
from jax import lax
from jax.sharding import PartitionSpec as P

IMG = 4096


low_taps = (
    -0.010597401784997278,
    0.032883011666982945,
    0.030841381835986965,
    -0.18703481171888114,
    -0.02798376941698385,
    0.6308807679295904,
    0.7148465705525415,
    0.23037781330885523,
)
high_taps = tuple(((-1.0) ** offset * low_taps[7 - offset] for offset in range(8)))
highest = lax.Precision.HIGHEST


def shifted(block, axis, distance):
    devices = range(lax.axis_size(axis))
    route = [((i - distance) % len(devices), i) for i in devices]
    return lax.ppermute(block, axis, route)


def dft_table(table_size, sign):
    positions = jnp.arange(table_size, dtype=jnp.int32)
    phase = positions[:, None] * positions[None, :] % table_size
    angle = 2.0 * math.pi / table_size * phase.astype(jnp.float32)
    return (jnp.cos(angle), sign * jnp.sin(angle))


def section_one(table, values):
    return jnp.einsum("kn,...nm->...km", table, values, precision=highest)


def section_two(table, values):
    return jnp.einsum("qm,...km->...qk", table, values, precision=highest)


def dft_last(real_in, imag_in, sign):
    leading = real_in.shape[:-1]
    length = real_in.shape[-1]
    inner_len = 64
    outer_len = length // inner_len
    split_real = real_in.reshape(leading + (outer_len, inner_len))
    table_real, table_imag = dft_table(outer_len, sign)
    first_real = section_one(table_real, split_real)
    first_imag = section_one(table_imag, split_real)
    if imag_in is not None:
        split_imag = imag_in.reshape(leading + (outer_len, inner_len))
        first_real = first_real - section_one(table_imag, split_imag)
        first_imag = first_imag + section_one(table_real, split_imag)
    outer_index = jnp.arange(outer_len, dtype=jnp.int32)
    inner_index = jnp.arange(inner_len, dtype=jnp.int32)
    twist_phase = outer_index[:, None] * inner_index[None, :] % length
    twist_angle = 2.0 * math.pi / length * twist_phase.astype(jnp.float32)
    twist_real = jnp.cos(twist_angle)
    twist_imag = sign * jnp.sin(twist_angle)
    mid_real = first_real * twist_real - first_imag * twist_imag
    mid_imag = first_real * twist_imag + first_imag * twist_real
    last_real, last_imag = dft_table(inner_len, sign)
    out_real = section_two(last_real, mid_real) - section_two(last_imag, mid_imag)
    out_imag = section_two(last_real, mid_imag) + section_two(last_imag, mid_real)
    factor = 1.0 / math.sqrt(length)
    return (
        (out_real * factor).reshape(leading + (length,)),
        (out_imag * factor).reshape(leading + (length,)),
    )


def pieces_from_image(extrap, band_count, group_count):
    rows_dev = extrap.shape[0]
    image_width = extrap.shape[1]
    stripe = image_width // band_count
    piece_cols = stripe // group_count
    piece_rows = image_width // group_count
    col_real, col_imag = dft_last(extrap, None, -1.0)
    shaped = jnp.stack([col_real, col_imag]).reshape(
        2, 1, 1, rows_dev, band_count, group_count, piece_cols
    )
    moved = lax.all_to_all(
        lax.all_to_all(shaped, "band", split_axis=4, concat_axis=1, tiled=True),
        "vis",
        split_axis=5,
        concat_axis=2,
        tiled=True,
    )
    columns = jnp.transpose(moved.reshape(2, image_width, piece_cols), (2, 0, 1))
    row_real, row_imag = dft_last(columns[:, 0], columns[:, 1], -1.0)
    stacked = (
        jnp.stack([row_real, row_imag], axis=1)
        .astype(jnp.bfloat16)
        .reshape(piece_cols, 2, group_count, piece_rows)
    )
    pieces = lax.all_to_all(stacked, "vis", split_axis=2, concat_axis=0, tiled=True)
    return pieces.reshape(stripe, 2, piece_rows)


def image_from_pieces(piece_sum, band_count, group_count):
    stripe = piece_sum.shape[0]
    piece_rows = piece_sum.shape[2]
    piece_cols = stripe // group_count
    image_width = piece_rows * group_count
    rows_dev = image_width // (band_count * group_count)
    spread = lax.all_to_all(
        piece_sum.reshape(stripe, 2, 1, piece_rows), "vis", split_axis=0, concat_axis=2, tiled=True
    )
    spread = spread.reshape(piece_cols, 2, image_width)
    col_real, col_imag = dft_last(spread[:, 0], spread[:, 1], 1.0)
    stacked = jnp.transpose(jnp.stack([col_real, col_imag]), (0, 2, 1))
    shaped = stacked.reshape(2, band_count, group_count, rows_dev, 1, 1, piece_cols)
    moved = lax.all_to_all(
        lax.all_to_all(shaped, "band", split_axis=1, concat_axis=4, tiled=True),
        "vis",
        split_axis=2,
        concat_axis=5,
        tiled=True,
    )
    moved = moved.reshape(2, rows_dev, image_width)
    out_real, out_imag = dft_last(moved[0], moved[1], 1.0)
    return out_real


def cols_down(field):
    image_width = field.shape[1]
    extended = jnp.concatenate([field, field[:, :6]], axis=1)
    low_part = 0.0
    high_part = 0.0
    for offset in range(8):
        taken = extended[:, offset : offset + image_width : 2]
        low_part = low_part + low_taps[offset] * taken
        high_part = high_part + high_taps[offset] * taken
    return (low_part, high_part)


def cols_up(low_part, high_part):
    halves = []
    for parity in range(2):
        summed = 0.0
        for delay in range(4):
            summed = summed + low_taps[parity + 2 * delay] * jnp.roll(low_part, delay, axis=1)
            summed = summed + high_taps[parity + 2 * delay] * jnp.roll(high_part, delay, axis=1)
        halves.append(summed)
    return jnp.stack(halves, axis=2).reshape(low_part.shape[0], 2 * low_part.shape[1])


def rows_up(low_ext, high_ext, half_rows):
    halves = []
    for parity in range(2):
        summed = 0.0
        for delay in range(4):
            begin = 3 - delay
            summed = summed + low_taps[parity + 2 * delay] * low_ext[begin : begin + half_rows]
            summed = summed + high_taps[parity + 2 * delay] * high_ext[begin : begin + half_rows]
        halves.append(summed)
    return jnp.stack(halves, axis=1).reshape(2 * half_rows, low_ext.shape[1])


def analysis(extrap):
    rows_dev = extrap.shape[0]
    taken_rows = min(6, rows_dev)
    parts_list = [extrap]
    parts_list.append(shifted(extrap[:taken_rows], ("band", "vis"), -1))
    extended = jnp.concatenate(parts_list, axis=0)
    half_rows = rows_dev // 2
    rows_low = 0.0
    rows_high = 0.0
    for offset in range(8):
        taken = extended[offset : offset + 2 * half_rows : 2]
        rows_low = rows_low + low_taps[offset] * taken
        rows_high = rows_high + high_taps[offset] * taken
    low_low, low_high = cols_down(rows_low)
    high_low, high_high = cols_down(rows_high)
    return jnp.stack([low_low, low_high, high_low, high_high])


def synthesis(coef_dual):
    half_rows = coef_dual.shape[1]
    taken_rows = min(3, half_rows)
    parts_list = [shifted(coef_dual[:, half_rows - taken_rows :, :], ("band", "vis"), 1)]
    joined = jnp.concatenate(parts_list[::-1] + [coef_dual], axis=1)
    cols_low = rows_up(joined[0], joined[2], half_rows)
    cols_high = rows_up(joined[1], joined[3], half_rows)
    return cols_up(cols_low, cols_high)


def degrid(kernel_here, tiles):
    kernel_real = kernel_here[:, :, 0]
    kernel_imag = kernel_here[:, :, 1]
    tile_real = tiles[:, :, 0]
    tile_imag = tiles[:, :, 1]
    out_real = jnp.einsum(
        "qsat,qst->qsa", kernel_real, tile_real, preferred_element_type=jnp.float32
    ) - jnp.einsum("qsat,qst->qsa", kernel_imag, tile_imag, preferred_element_type=jnp.float32)
    out_imag = jnp.einsum(
        "qsat,qst->qsa", kernel_real, tile_imag, preferred_element_type=jnp.float32
    ) + jnp.einsum("qsat,qst->qsa", kernel_imag, tile_real, preferred_element_type=jnp.float32)
    return jnp.stack([out_real, out_imag], axis=2)


def grid_back(kernel_here, weights):
    kernel_real = kernel_here[:, :, 0]
    kernel_imag = kernel_here[:, :, 1]
    weight_real = weights[:, :, 0]
    weight_imag = weights[:, :, 1]
    grid_real = jnp.einsum(
        "qsat,qsa->qst", kernel_real, weight_real, preferred_element_type=jnp.float32
    ) + jnp.einsum("qsat,qsa->qst", kernel_imag, weight_imag, preferred_element_type=jnp.float32)
    grid_imag = jnp.einsum(
        "qsat,qsa->qst", kernel_real, weight_imag, preferred_element_type=jnp.float32
    ) - jnp.einsum("qsat,qsa->qst", kernel_imag, weight_real, preferred_element_type=jnp.float32)
    return jnp.stack([grid_real, grid_imag], axis=2)


def local(sky_image, coef_dual, vis_dual, visibilities, kernel_blocks, tile_rows, tile_counts):
    band_count = lax.axis_size("band")
    group_count = lax.axis_size("vis")
    kernel_here = kernel_blocks[0, 0]
    rows_here = tile_rows[0, 0]
    slot_count = rows_here.shape[1]
    live_slots = (
        jnp.arange(slot_count, dtype=jnp.int32)[None, :] < tile_counts[0, 0][:, None]
    ).astype(jnp.float32)[:, :, None, None]
    vis_data = visibilities[0, 0]
    vis_state = vis_dual[0, 0]
    image_width = sky_image.shape[1]
    stripe = image_width // band_count
    piece_rows = image_width // group_count
    incoming_rows = lax.all_to_all(rows_here, "vis", split_axis=0, concat_axis=0, tiled=True)
    data_part = jnp.sum(live_slots * vis_data * vis_data)
    weights = (live_slots * vis_state).astype(jnp.bfloat16)
    contrib = grid_back(kernel_here, weights)
    arrived = lax.all_to_all(contrib, "vis", split_axis=0, concat_axis=0, tiled=True)
    piece_sum = jax.ops.segment_sum(
        arrived.reshape(-1, 2, piece_rows), incoming_rows.reshape(-1), num_segments=stripe
    )
    adjoint_part = image_from_pieces(piece_sum, band_count, group_count)
    smooth = synthesis(coef_dual)
    new_image = jnp.maximum(sky_image - smooth - adjoint_part, 0.0)
    extrap = 2.0 * new_image - sky_image
    coeffs = analysis(extrap)
    abs_total = jnp.sum(jnp.abs(coeffs))
    coef_total = lax.psum(abs_total, ("band", "vis"))
    threshold = 0.5 * coef_total / (IMG * IMG)
    coef_dual = jnp.clip(coef_dual + coeffs, -threshold, threshold)
    piece_grid = pieces_from_image(extrap, band_count, group_count)
    tiles = lax.all_to_all(
        piece_grid[incoming_rows], "vis", split_axis=0, concat_axis=0, tiled=True
    )
    predicted = degrid(kernel_here, tiles)
    residual = live_slots * (vis_state + predicted - vis_data)
    resid_square = jnp.sum(residual * residual)
    norm_square, data_square = lax.psum((resid_square, data_part), ("band", "vis"))
    radius = 0.5 * jnp.sqrt(data_square + 1e-06)
    size_value = jnp.sqrt(norm_square + 1e-06)
    vis_state = residual * (1.0 - jnp.minimum(1.0, radius / size_value))
    return (new_image, coef_dual, vis_state[None, None])


high = lax.Precision.HIGH
everywhere = ("band", "vis")


def wave_tables(length, digit_low):
    digit_high = length // digit_low
    low = np.arange(digit_low)
    wide = np.arange(digit_high)
    full = 2.0 * np.pi
    small = full * (low[:, None] * low[None, :] % digit_low) / digit_low
    twist = full * (low[:, None] * wide[None, :]) / length
    large = full * (wide[:, None] * wide[None, :] % digit_high) / digit_high
    return small, twist, large


def complex_matrix(angle, sign):
    c = np.cos(angle)
    s = sign * np.sin(angle)
    return np.stack([np.stack([c, -s], axis=1), np.stack([s, c], axis=1)])


def f32(values):
    return jnp.asarray(np.asarray(values, np.float32))


def bf16(values):
    return f32(values).astype(jnp.bfloat16)


def analysis_matrix(half):
    matrix = np.zeros((2, half, 2 * half + 6))
    for k in range(half):
        for j in range(8):
            matrix[0, k, 2 * k + j] = low_taps[j]
            matrix[1, k, 2 * k + j] = high_taps[j]
    return matrix.reshape(2 * half, 2 * half + 6)


def synthesis_matrix(half):
    matrix = np.zeros((2 * half, 2, half + 3))
    for n in range(2 * half):
        for delay in range(4):
            tap = n % 2 + 2 * delay
            matrix[n, 0, n // 2 - delay + 3] = low_taps[tap]
            matrix[n, 1, n // 2 - delay + 3] = high_taps[tap]
    return matrix


def fast_analysis(extrap):
    rows_dev, width = extrap.shape
    halo = shifted(extrap[:6], everywhere, -1)
    extended = jnp.concatenate([extrap, halo], axis=0)
    by_rows = jnp.einsum("ij,jn->in", f32(analysis_matrix(rows_dev // 2)), extended, precision=high)
    size = 256
    blocks = by_rows.reshape(rows_dev, width // size, size)
    following = jnp.roll(blocks, -1, axis=1)[:, :, :6]
    matrix = analysis_matrix(size // 2)
    out = jnp.einsum("rbi,ji->rbj", blocks, f32(matrix[:, :size]), precision=high)
    out = out + jnp.einsum("rbi,ji->rbj", following, f32(matrix[:, size:]), precision=high)
    out = out.reshape(2, rows_dev // 2, width // size, 2, size // 2)
    return jnp.transpose(out, (0, 3, 1, 2, 4)).reshape(4, rows_dev // 2, width // 2)


def fast_synthesis(coef_dual):
    half_rows, half_width = coef_dual.shape[1:]
    halo = shifted(coef_dual[:, half_rows - 3 :, :], everywhere, 1)
    joined = jnp.concatenate([halo, coef_dual], axis=1)
    joined = joined.reshape(2, 2, half_rows + 3, half_width)
    by_rows = jnp.einsum("irj,rcjn->cin", f32(synthesis_matrix(half_rows)), joined, precision=high)
    size = 128
    blocks = by_rows.reshape(2, 2 * half_rows, half_width // size, size)
    before = jnp.roll(blocks, 1, axis=2)[:, :, :, size - 3 :]
    matrix = synthesis_matrix(size)
    out = jnp.einsum("cibk,nck->ibn", blocks, f32(matrix[:, :, 3:]), precision=high)
    out = out + jnp.einsum("cibk,nck->ibn", before, f32(matrix[:, :, :3]), precision=high)
    return out.reshape(2 * half_rows, 2 * half_width)


def fold_plan(width, devices):
    wide = 128
    low = width // wide
    return wide, low, low // 2 + 1, wide // devices


def column_of(columns, low, kept, each, wide):
    k1 = columns % low
    k2 = columns // low
    k2 = jnp.where(k1 < kept, k2, wide - 1 - k2)
    return k2 // each, k1 * each + k2 % each


def forward_columns(extrap, devices):
    rows_dev, width = extrap.shape
    wide, low, kept, each = fold_plan(width, devices)
    small, twist, large = wave_tables(width, low)
    scale = 1.0 / math.sqrt(width)
    first = complex_matrix(small, -1.0)[:, :kept, 0, :]
    mid = jnp.einsum("pka,mac->pkmc", f32(first), extrap.reshape(rows_dev, low, wide), precision=high)
    tw_real = f32(np.cos(twist))[:kept, None, :]
    tw_imag = f32(-np.sin(twist))[:kept, None, :]
    turned = jnp.concatenate(
        [mid[0] * tw_real - mid[1] * tw_imag, mid[0] * tw_imag + mid[1] * tw_real], axis=-1
    )
    last = scale * complex_matrix(large, -1.0)
    last = last.reshape(2, devices, each, 2 * wide).transpose(1, 0, 2, 3).reshape(2 * wide, 2 * wide)
    out = jnp.einsum("kmx,px->kpm", turned, f32(last), precision=high)
    out = out.reshape(kept, devices, 2, each, rows_dev).transpose(1, 2, 0, 3, 4)
    out = out.reshape(devices, 2, kept * each, rows_dev)
    got = lax.all_to_all(out, everywhere, split_axis=0, concat_axis=0, tiled=True)
    split = got.reshape(devices, 2, kept, each, rows_dev)
    sign = f32([1.0, -1.0])[None, :, None, None, None]
    mirror = split[:, :, 1 : kept - 1][:, :, ::-1] * sign
    columns = jnp.concatenate([split, mirror], axis=2)
    columns = columns.reshape(2 * devices, low * each, rows_dev)
    small, twist, large = wave_tables(width, devices)
    first = complex_matrix(small, -1.0).transpose(0, 1, 3, 2)
    mid = jnp.einsum(
        "pq,qcm->pcm", f32(first.reshape(2 * devices, 2 * devices)), columns, precision=high
    ).reshape(2, devices, low * each, rows_dev)
    tw_real = f32(np.cos(twist))[:, None, :]
    tw_imag = f32(-np.sin(twist))[:, None, :]
    turned = jnp.concatenate(
        [mid[0] * tw_real - mid[1] * tw_imag, mid[0] * tw_imag + mid[1] * tw_real], axis=-1
    )
    return turned, scale * complex_matrix(large, -1.0)


def image_rows(grid, devices, groups, width):
    rows_dev = width // devices
    wide, low, kept, each = fold_plan(width, devices)
    small, twist, large = wave_tables(width, devices)
    scale = 1.0 / math.sqrt(width)
    first = scale * complex_matrix(large, 1.0)
    first = first.reshape(2 * rows_dev, 2, groups, rows_dev // groups).transpose(0, 2, 1, 3)
    mid = jnp.einsum(
        "fpc,xp->fcx",
        grid,
        bf16(first.reshape(2 * rows_dev, 2 * rows_dev)),
        preferred_element_type=jnp.float32,
    )
    tw_real = f32(np.cos(twist))[:, None, :]
    tw_imag = f32(np.sin(twist))[:, None, :]
    mid_real, mid_imag = mid[..., :rows_dev], mid[..., rows_dev:]
    turned = jnp.stack(
        [mid_real * tw_real - mid_imag * tw_imag, mid_real * tw_imag + mid_imag * tw_real]
    ).astype(jnp.bfloat16)
    turned = turned.reshape(2 * devices, low * each, rows_dev)
    second = complex_matrix(small, 1.0).transpose(1, 0, 2, 3)
    out = jnp.einsum(
        "pq,qcm->pcm",
        bf16(second.reshape(2 * devices, 2 * devices)),
        turned,
        preferred_element_type=jnp.float32,
    ).reshape(devices, 2, low, each, rows_dev)
    sign = f32([1.0, -1.0])[None, :, None, None, None]
    folded = out[:, :, kept:][:, :, ::-1] * sign
    folded = jnp.pad(folded, ((0, 0), (0, 0), (1, 1), (0, 0), (0, 0)))
    send = (out[:, :, :kept] + folded).astype(jnp.bfloat16)
    send = send.reshape(devices, 2, kept * each, rows_dev)
    got = lax.all_to_all(send, everywhere, split_axis=0, concat_axis=0, tiled=True)
    got = got.reshape(devices, 2, kept, each, rows_dev).transpose(2, 0, 1, 3, 4)
    got = got.reshape(kept, 2 * wide, rows_dev)
    small, twist, large = wave_tables(width, low)
    first = scale * complex_matrix(large, 1.0)
    first = first.reshape(2 * wide, 2, devices, each).transpose(0, 2, 1, 3)
    mid = jnp.einsum(
        "kpm,xp->kmx",
        got,
        bf16(first.reshape(2 * wide, 2 * wide)),
        preferred_element_type=jnp.float32,
    )
    tw_real = f32(np.cos(twist))[:kept, None, :]
    tw_imag = f32(np.sin(twist))[:kept, None, :]
    mid_real, mid_imag = mid[..., :wide], mid[..., wide:]
    turned = jnp.stack(
        [mid_real * tw_real - mid_imag * tw_imag, mid_real * tw_imag + mid_imag * tw_real]
    ).astype(jnp.bfloat16)
    second = complex_matrix(small, 1.0)[0][:, :, :kept]
    out = jnp.einsum(
        "apk,pkmc->mac", bf16(second), turned, preferred_element_type=jnp.float32
    )
    return out.reshape(rows_dev, width)


def to_all(values, devices):
    flat = jnp.broadcast_to(values.reshape(1, -1), (devices, values.size))
    return lax.all_to_all(flat, everywhere, split_axis=0, concat_axis=0, tiled=True)


def halving_steps(bands, groups):
    steps = [("band", bit) for bit in range(bands.bit_length() - 1)]
    steps += [("vis", bit) for bit in range(1, groups.bit_length() - 1)]
    return [("vis", 0)] + steps


def slot_order(steps, bands, groups):
    order = []
    for code in range(bands * groups):
        index = {"band": 0, "vis": 0}
        for depth, (axis, bit) in enumerate(steps):
            index[axis] |= (code >> (len(steps) - 1 - depth) & 1) << bit
        order.append(index["band"] * groups + index["vis"])
    return order


def halved(values, steps):
    for axis, bit in steps:
        mine = (lax.axis_index(axis) >> bit) & 1
        half = values.shape[1] // 2
        first, second = values[:, :half], values[:, half:]
        route = [(i, i ^ (1 << bit)) for i in range(lax.axis_size(axis))]
        got = lax.ppermute(jnp.where(mine == 1, first, second), axis, route)
        values = jnp.where(mine == 1, second, first) + got
    return values


def fast_local(sky_image, coef_dual, vis_dual, visibilities, kernel_blocks, tile_rows, tile_counts):
    bands = lax.axis_size("band")
    groups = lax.axis_size("vis")
    devices = bands * groups
    me = lax.axis_index(everywhere)
    kernel_here = kernel_blocks[0, 0]
    slots = tile_rows.shape[3]
    rows_dev, width = sky_image.shape
    piece = width // groups
    stripe = width // bands
    wide, low, kept, each = fold_plan(width, devices)
    near = piece // devices
    live_slots = (
        jnp.arange(slots, dtype=jnp.int32)[None, :] < tile_counts[0, 0][:, None]
    ).astype(jnp.float32)[:, :, None, None]
    vis_data = visibilities[0, 0]
    vis_state = vis_dual[0, 0]
    columns_here = tile_rows[0, 0] + lax.axis_index("band") * stripe
    columns_all = to_all(columns_here, devices).reshape(devices, groups, slots)
    steps = halving_steps(bands, groups)
    order = slot_order(steps, bands, groups)
    columns_cut = jnp.concatenate([columns_all[i : i + 1] for i in order], axis=0)

    def one_hot(columns):
        columns = columns.transpose(1, 0, 2).reshape(groups, -1)
        holder, place = column_of(columns, low, kept, each, wide)
        hit = place[:, :, None] == jnp.arange(low * each, dtype=jnp.int32)
        return ((holder == me)[:, :, None] & hit).astype(jnp.bfloat16)

    weights = (live_slots * vis_state).astype(jnp.bfloat16)
    contrib = grid_back(kernel_here, weights).astype(jnp.bfloat16)
    contrib = contrib.reshape(groups, slots, 2, near, devices).transpose(0, 1, 4, 2, 3)
    contrib = contrib.reshape(groups, slots, 2 * piece)
    gathered = lax.all_gather(contrib, everywhere)
    gathered = gathered.transpose(1, 0, 2, 3).reshape(groups, devices * slots, 2 * piece)
    grid = jnp.einsum("qsx,qsc->qxc", gathered, one_hot(columns_all), preferred_element_type=jnp.float32)
    grid = grid.astype(jnp.bfloat16).reshape(groups, devices, 2 * near, low * each)
    grid = grid.transpose(1, 0, 2, 3).reshape(devices, groups * 2 * near, low * each)
    adjoint_part = image_rows(grid, devices, groups, width)
    smooth = fast_synthesis(coef_dual)
    new_image = jnp.maximum(sky_image - smooth - adjoint_part, 0.0)
    extrap = 2.0 * new_image - sky_image
    turned, last = forward_columns(extrap, devices)
    last = last.reshape(2, groups, near, 2 * rows_dev).transpose(1, 0, 2, 3)
    last = last.reshape(2 * rows_dev, 2 * rows_dev)
    spec = jnp.einsum("fcx,px->fpc", turned, f32(last), precision=high).astype(jnp.bfloat16)
    spec = spec.reshape(devices, groups, 2 * near, low * each).transpose(1, 0, 2, 3)
    spec = spec.reshape(groups, 2 * piece, low * each)
    picked = jnp.einsum("qsc,qxc->qsx", one_hot(columns_cut), spec, preferred_element_type=jnp.float32)
    tiles = halved(picked.astype(jnp.bfloat16), steps)
    tiles = tiles.reshape(groups, slots, devices, 2, near).transpose(0, 1, 3, 4, 2)
    tiles = tiles.reshape(groups, slots, 2, piece)
    coeffs = fast_analysis(extrap)
    predicted = degrid(kernel_here, tiles)
    residual = live_slots * (vis_state + predicted - vis_data)
    sums = jnp.stack(
        [
            jnp.sum(jnp.abs(coeffs)),
            jnp.sum(residual * residual),
            jnp.sum(live_slots * vis_data * vis_data),
        ]
    )
    sums = jnp.sum(to_all(sums, devices), axis=0)
    threshold = 0.5 * sums[0] / (width * width)
    coef_dual = jnp.clip(coef_dual + coeffs, -threshold, threshold)
    radius = 0.5 * jnp.sqrt(sums[2] + 1e-06)
    size_value = jnp.sqrt(sums[1] + 1e-06)
    vis_state = residual * (1.0 - jnp.minimum(1.0, radius / size_value))
    return (new_image, coef_dual, vis_state[None, None])


def body_for(mesh):
    devices = mesh.shape["band"] * mesh.shape["vis"]

    def body(sky_image, *rest):
        if sky_image.shape[0] == 128 and 128 % devices == 0:
            return fast_local(sky_image, *rest)
        return local(sky_image, *rest)

    return body


def solution(mesh):
    return jax.shard_map(
        body_for(mesh),
        mesh=mesh,
        in_specs=(
            P(("band", "vis"), None),
            P(None, ("band", "vis"), None),
            P("band", "vis", None, None, None, None),
            P("band", "vis", None, None, None, None),
            P("band", "vis", None, None, None, None, None),
            P("band", "vis", None, None),
            P("band", "vis", None),
        ),
        out_specs=(
            P(("band", "vis"), None),
            P(None, ("band", "vis"), None),
            P("band", "vis", None, None, None, None),
        ),
        check_vma=False,
    )
```
